32 devices in a mesh: cells: 8 (over z, y), coef: 4 (over x, core).
Axes of the slice: x: 2, y: 2, z: 4, core: 2. Of those that a mesh axis runs over, the one named last changes fastest.
Arguments:
- multipole: bfloat16 [128, 1024], P('coef', 'cells'), may hold values from -6 to 6
- parent_local: bfloat16 [128, 128], P('coef', 'cells'), may hold values from -6 to 6
- m2l_ops: bfloat16 [189, 128, 128], P(None, 'coef'), may hold values from -0.0390625 to 0.0390625
- l2l_ops: bfloat16 [8, 128, 128], P(None, 'coef'), may hold values from -0.5 to 0.5
- target_cell: int32 [189, 1024], P(None, 'cells'), may hold values from -1 to 1023, as said below
- particle_leaf: int32 [16384], P('cells'), may hold values from 0 to 1023, as said below
- particle_basis: bfloat16 [128, 16384], P('coef', 'cells'), may hold values from -0.5 to 0.5
Outputs:
- leaf_local: float32 [128, 1024], P('coef', 'cells')
- potential: float32 [16384], P('cells')
The draws below stay inside these ranges and needn't reach their ends.
Inputs may be any that keep to these rules, and one draw needn't show every extreme that they name: `target_cell`: -1 marks an empty slot. Otherwise the target of source cell c lies on the device of c (cells are owned in blocks of 128: device c // 128) or on a device at most 2 indices away; from one device's source cells at most 256 pairs target the cells of any one other device, and some pair of devices has exactly 256. `particle_leaf`: the particles at positions d * 2048 to (d + 1) * 2048 - 1 lie in cells d * 128 to (d + 1) * 128 - 1.
All inputs are finite; a program needn't handle non-finite values.
Results may differ from the reference program's by a relative error of at most 0.0003.
Values may be sent and summed in bfloat16 or wider, within the bound.
A program may use at most 64 MiB of HBM per device.

```python
import jax
import jax.numpy as jnp
import numpy as np
from jax import lax

K = 128
NOFF = 189
CD = 128
PD = 2048
CAP = 256
REACH = 2
OWNERS = 8
CELLS = 1024
PCELLS = 128
PARTICLES = 16384


def draw_target_cell(key, part):
    moves = jnp.asarray(np.concatenate([np.arange(-REACH, 0), np.arange(1, REACH + 1)]), jnp.int32)
    groups = 2 * REACH
    pairs = NOFF * CD

    def one_device(device):
        device_key = jax.random.fold_in(jax.random.fold_in(key, 11), device)
        keys = jax.random.split(device_key, 5)
        counts = jax.random.randint(keys[0], (groups,), CAP // 4, CAP + 1)
        forced = jax.random.randint(keys[1], (), 0, groups)
        counts = jnp.where(jnp.arange(groups) == forced, CAP, counts)
        dests = device + moves
        inside = (dests >= 0) & (dests < OWNERS)
        counts = jnp.where(inside, counts, 0).astype(jnp.int32)
        ends = jnp.cumsum(counts).astype(jnp.int32)
        order = jax.random.permutation(keys[2], pairs)
        place = jnp.zeros((pairs,), jnp.int32).at[order].set(jnp.arange(pairs, dtype=jnp.int32))
        group = jnp.searchsorted(ends, place, side='right').astype(jnp.int32)
        remote = group < groups
        target_dev = device + moves[jnp.minimum(group, groups - 1)]
        cell = jax.random.randint(keys[3], (pairs,), 0, CD)
        empty = jax.random.randint(keys[4], (pairs,), 0, 8) == 0
        local_target = jnp.where(empty, -1, device * CD + cell)
        result = jnp.where(remote, target_dev * CD + cell, local_target)
        return result.astype(jnp.int32).reshape(NOFF, CD)
    table = lax.map(one_device, jnp.arange(OWNERS, dtype=jnp.int32))
    return jnp.transpose(table, (1, 0, 2)).reshape(NOFF, OWNERS * CD)


def draw_particle_leaf(key, part):
    leaf_key = jax.random.fold_in(key, 23)
    owner = jnp.arange(PD * OWNERS, dtype=jnp.int32) // PD
    cell = jax.random.randint(leaf_key, (PD * OWNERS,), 0, CD)
    return (owner * CD + cell).astype(jnp.int32)


def block_scale(own_key, extent, pieces, smallest, largest):
    gain = 1.0
    for dim, parts in pieces:
        steps = jax.random.uniform(jax.random.fold_in(jax.random.fold_in(own_key, 6), dim), (parts,), jnp.float32, smallest / len(pieces), largest / len(pieces))
        gain = gain * jnp.repeat(jnp.exp(steps), extent[dim] // parts).reshape((-1,) + (1,) * (len(extent) - 1 - dim))
    return gain


def normal_values(stream_key, dims, scale, bound, shards=(), kind=jnp.bfloat16):
    loudness = block_scale(stream_key, dims, shards, -0.22, 0.18) if shards else 1.0
    values = jax.random.normal(stream_key, dims, jnp.float32) * scale * loudness
    return jnp.minimum(jnp.maximum(values, -bound), bound).astype(kind)


def setup_inputs(seed: int = 0) -> dict:
    key_list = jax.random.split(jax.random.key(seed), 8)
    multipole = normal_values(key_list[0], (K, CELLS), 1.0, 6.0, ((0, 4), (1, 8)))
    parent_local = normal_values(key_list[1], (K, PCELLS), 1.0, 6.0, ((0, 4), (1, 8)))
    m2l_ops = normal_values(key_list[2], (NOFF, K, K), (K * NOFF) ** -0.5, 0.0390625, ((1, 4),))
    l2l_ops = normal_values(key_list[3], (8, K, K), K ** -0.5, 0.5, ((1, 4),))
    target_cell = draw_target_cell(jax.random.fold_in(key_list[7], 71), 0)
    particle_leaf = draw_particle_leaf(jax.random.fold_in(key_list[7], 71), 0)
    particle_basis = normal_values(key_list[6], (K, PARTICLES), K ** -0.5, 0.5, ((0, 4), (1, 8)))
    return dict(multipole=multipole, parent_local=parent_local, m2l_ops=m2l_ops, l2l_ops=l2l_ops, target_cell=target_cell, particle_leaf=particle_leaf, particle_basis=particle_basis)


def reference(multipole, parent_local, m2l_ops, l2l_ops, target_cell, particle_leaf, particle_basis):
    width = multipole.shape[0]
    cell_count = multipole.shape[1]
    poles_wide = multipole.astype(jnp.float32)
    parents_wide = parent_local.astype(jnp.float32)

    def offset_step(total, inputs):
        operator, targets = inputs
        term = jnp.dot(operator.astype(jnp.float32), poles_wide, preferred_element_type=jnp.float32)
        index = jnp.where(targets >= 0, targets, cell_count).astype(jnp.int32)
        return total.at[:, index].add(term, mode="drop"), None

    start = jnp.zeros((width, cell_count), jnp.float32)
    m2l_sum, _ = lax.scan(offset_step, start, (m2l_ops, target_cell))
    children = [jnp.dot(l2l_ops[octant].astype(jnp.float32), parents_wide, preferred_element_type=jnp.float32) for octant in range(8)]
    shifted = jnp.stack(children, axis=2).reshape(width, cell_count)
    leaf_local = m2l_sum + shifted
    columns = leaf_local[:, particle_leaf]
    potential = jnp.sum(columns * particle_basis.astype(jnp.float32), axis=0)
    return leaf_local, potential
```

```python
import functools

import jax
import jax.numpy as jnp
from jax import lax
from jax.experimental import pallas as pl
from jax.experimental.pallas import tpu as pltpu
from jax.sharding import PartitionSpec as P

REACH = 2
WINDOWS = tuple(w for r in range(REACH, 0, -1) for w in (-r, r))
GROUP = 16
NT = (((1,), (1,)), ((), ()))


def halves(value):
    high = value.astype(jnp.bfloat16)
    low = (value - high.astype(jnp.float32)).astype(jnp.bfloat16)
    return high, low


def kernel(
    n_cells, n_coef,
    mine_ref, ops_hbm, l2l_hbm, target_hbm, leaf_hbm, basis_hbm,
    local_ref, pot_ref,
    ops_ref, l2l_ref, target_ref, leaf_ref, basis_ref,
    gathered, pieces, out_buf, in_buf, total, partials,
    load_sem, g_send, g_recv, w_send, w_recv, p_send, p_recv,
):
    row = lax.axis_index("cells")
    col = lax.axis_index("coef")
    noff, share, width = ops_ref.shape
    cd = target_ref.shape[1]
    tiles = leaf_ref.shape[0]
    lanes = leaf_ref.shape[1]

    loads = [
        pltpu.make_async_copy(src, dst, load_sem.at[i])
        for i, (src, dst) in enumerate(
            ((target_hbm, target_ref), (ops_hbm, ops_ref), (l2l_hbm, l2l_ref),
             (leaf_hbm, leaf_ref), (basis_hbm, basis_ref))
        )
    ]
    for load in loads:
        load.start()

    barrier = pltpu.get_barrier_semaphore()
    for d in range(1, n_coef):
        pl.semaphore_signal(
            barrier, inc=1, device_id=(row, lax.rem(col + d, n_coef)),
            device_id_type=pl.DeviceIdType.MESH,
        )
    for w in WINDOWS:
        @pl.when((row + w >= 0) & (row + w < n_cells))
        def _():
            pl.semaphore_signal(
                barrier, inc=1, device_id=(row + w, col), device_id_type=pl.DeviceIdType.MESH
            )
    peers = n_coef - 1
    for w in WINDOWS:
        peers = peers + ((row + w >= 0) & (row + w < n_cells)).astype(jnp.int32)
    pl.semaphore_wait(barrier, peers)

    def gather_copy(d):
        return pltpu.make_async_remote_copy(
            src_ref=mine_ref, dst_ref=gathered.at[col],
            send_sem=g_send.at[d - 1], recv_sem=g_recv.at[col],
            device_id=(row, lax.rem(col + d, n_coef)), device_id_type=pl.DeviceIdType.MESH,
        )

    def gather_arrival(d):
        source = lax.rem(col + d, n_coef)
        return pltpu.make_async_remote_copy(
            src_ref=mine_ref, dst_ref=gathered.at[source],
            send_sem=g_send.at[d - 1], recv_sem=g_recv.at[source],
            device_id=(row, source), device_id_type=pl.DeviceIdType.MESH,
        )

    for d in range(1, n_coef):
        gather_copy(d).start()
    gathered[col] = mine_ref[...]
    loads[0].wait()
    loads[1].wait()
    for d in range(1, n_coef):
        gather_arrival(d).wait_recv()

    poles = jnp.concatenate([gathered[j, :, :cd] for j in range(n_coef)], axis=0)
    iota = lax.broadcasted_iota(jnp.int32, (cd, cd), 0).astype(jnp.float32).astype(jnp.bfloat16)
    one = jnp.ones((cd, cd), jnp.bfloat16)
    zero = jnp.zeros((cd, cd), jnp.bfloat16)

    def one_hot(line):
        wide = jnp.broadcast_to(line.astype(jnp.float32), (16, line.shape[1])).astype(jnp.bfloat16)
        tall = jnp.concatenate([wide] * (cd // 16), axis=0)
        return jnp.where(tall == iota, one, zero)

    def lines(first, count):
        result = []
        for j in range(count):
            line = target_ref[pl.ds(first + j, 1), :]
            result.append(jnp.where(line >= 0, line - row * cd, -8 * REACH * cd))
        return result

    def span(first, count):
        return pl.ds(pl.multiple_of(first * cd, cd), count * cd)

    def far(first, count):
        block = ops_ref[pl.ds(first, count)].reshape(count * share, width)
        terms = jnp.dot(block, poles, preferred_element_type=jnp.float32)
        high, low = halves(terms)
        both = jnp.concatenate(
            [
                jnp.concatenate([part[j * share : (j + 1) * share] for j in range(count)], axis=1)
                for part in (high, low)
            ],
            axis=0,
        )
        pieces[:, span(first, count)] = both
        rows = lines(first, count)
        hot = jnp.concatenate(
            [
                jnp.concatenate([one_hot(line - w * cd) for line in rows], axis=1)
                for w in WINDOWS
            ],
            axis=0,
        )
        return lax.dot_general(both, hot, NT, preferred_element_type=jnp.float32)

    def near(first, count):
        hot = jnp.concatenate([one_hot(line) for line in lines(first, count)], axis=1)
        return lax.dot_general(
            pieces[:, span(first, count)], hot, NT, preferred_element_type=jnp.float32
        )

    def over_offsets(step, columns):
        full = noff // GROUP
        acc = jnp.zeros((2 * share, columns), jnp.float32)
        acc = lax.fori_loop(0, full, lambda i, a: a + step(i * GROUP, GROUP), acc)
        if noff % GROUP:
            acc = acc + step(full * GROUP, noff % GROUP)
        return acc[:share] + acc[share:]

    def window_copy(i, w):
        return pltpu.make_async_remote_copy(
            src_ref=out_buf.at[i], dst_ref=in_buf.at[i],
            send_sem=w_send.at[i], recv_sem=w_recv.at[i],
            device_id=(row + w, col), device_id_type=pl.DeviceIdType.MESH,
        )

    sums = over_offsets(far, len(WINDOWS) * cd)
    for i, w in enumerate(WINDOWS):
        out_buf[i] = sums[:, i * cd : (i + 1) * cd]
    for i, w in enumerate(WINDOWS):
        @pl.when((row + w >= 0) & (row + w < n_cells))
        def _():
            window_copy(i, w).start()

    total[...] = over_offsets(near, cd)

    loads[2].wait()
    parents = jnp.concatenate([gathered[j, :, cd:] for j in range(n_coef)], axis=0)
    octant = lax.broadcasted_iota(jnp.int32, parents.shape, 1) % 8
    wide_parents = parents.astype(jnp.float32)
    spread = jnp.concatenate(
        [jnp.where(octant == j, wide_parents, 0.0).astype(jnp.bfloat16) for j in range(8)], axis=0
    )
    shifts = jnp.concatenate([l2l_ref[j] for j in range(8)], axis=1)
    total[...] += jnp.dot(shifts, spread, preferred_element_type=jnp.float32)

    loads[3].wait()
    leaf_hot = jnp.concatenate(
        [one_hot(leaf_ref[t : t + 1, :] - row * cd) for t in range(tiles)], axis=1
    )
    loads[4].wait()

    for i, w in enumerate(WINDOWS):
        @pl.when((row - w >= 0) & (row - w < n_cells))
        def _():
            window_copy(i, w).wait_recv()
            total[...] += in_buf[i]

    local = total[...]
    local_ref[...] = local
    columns = jnp.dot(
        jnp.concatenate(halves(local), axis=0), leaf_hot, preferred_element_type=jnp.float32
    )
    columns = columns[:share] + columns[share:]
    partial = jnp.sum(columns * basis_ref[...].astype(jnp.float32), axis=0, keepdims=True)
    partials[col] = jnp.concatenate(
        [partial[:, t * lanes : (t + 1) * lanes] for t in range(tiles)], axis=0
    )

    def partial_copy(d, slot):
        return pltpu.make_async_remote_copy(
            src_ref=partials.at[slot], dst_ref=partials.at[slot],
            send_sem=p_send.at[d - 1], recv_sem=p_recv.at[slot],
            device_id=(row, lax.rem(col + d, n_coef)), device_id_type=pl.DeviceIdType.MESH,
        )

    for d in range(1, n_coef):
        partial_copy(d, col).start()
    for d in range(1, n_coef):
        partial_copy(d, lax.rem(col + d, n_coef)).wait_recv()
    potential = partials[0]
    for j in range(1, n_coef):
        potential = potential + partials[j]
    pot_ref[...] = potential

    for d in range(1, n_coef):
        gather_copy(d).wait_send()
        partial_copy(d, col).wait_send()
    for i, w in enumerate(WINDOWS):
        @pl.when((row + w >= 0) & (row + w < n_cells))
        def _():
            window_copy(i, w).wait_send()


def on_device(
    n_cells, n_coef,
    multipole, parent_local, m2l_ops, l2l_ops, target_cell, particle_leaf, particle_basis,
):
    share, cd = multipole.shape
    noff = m2l_ops.shape[0]
    width = m2l_ops.shape[2]
    particles = particle_leaf.shape[0]
    lanes = 128
    tiles = particles // lanes
    mine = jnp.concatenate([multipole, jnp.repeat(parent_local, 8, axis=1)], axis=1)
    leaf = particle_leaf.reshape(tiles, lanes)
    nwin = len(WINDOWS)
    dma = pltpu.SemaphoreType.DMA
    vmem = pl.BlockSpec(memory_space=pltpu.VMEM)
    anywhere = pl.BlockSpec(memory_space=pl.ANY)
    local, potential = pl.pallas_call(
        functools.partial(kernel, n_cells, n_coef),
        out_shape=(
            jax.ShapeDtypeStruct((share, cd), jnp.float32),
            jax.ShapeDtypeStruct((tiles, lanes), jnp.float32),
        ),
        in_specs=[vmem] + [anywhere] * 5,
        out_specs=(vmem, vmem),
        scratch_shapes=[
            pltpu.VMEM(m2l_ops.shape, m2l_ops.dtype),
            pltpu.VMEM(l2l_ops.shape, l2l_ops.dtype),
            pltpu.VMEM(target_cell.shape, target_cell.dtype),
            pltpu.VMEM(leaf.shape, leaf.dtype),
            pltpu.VMEM(particle_basis.shape, particle_basis.dtype),
            pltpu.VMEM((n_coef, share, 2 * cd), jnp.bfloat16),
            pltpu.VMEM((2 * share, noff * cd), jnp.bfloat16),
            pltpu.VMEM((nwin, share, cd), jnp.float32),
            pltpu.VMEM((nwin, share, cd), jnp.float32),
            pltpu.VMEM((share, cd), jnp.float32),
            pltpu.VMEM((n_coef, tiles, lanes), jnp.float32),
            dma((5,)),
            dma((n_coef - 1,)),
            dma((n_coef,)),
            dma((nwin,)),
            dma((nwin,)),
            dma((n_coef - 1,)),
            dma((n_coef,)),
        ],
        compiler_params=pltpu.CompilerParams(
            collective_id=0, has_side_effects=True, vmem_limit_bytes=48 * 1024 * 1024
        ),
    )(mine, m2l_ops, l2l_ops, target_cell, leaf, particle_basis)
    return local, potential.reshape(particles)


def solution(mesh):
    return jax.shard_map(
        functools.partial(on_device, mesh.shape["cells"], mesh.shape["coef"]),
        mesh=mesh,
        in_specs=(
            P("coef", "cells"),
            P("coef", "cells"),
            P(None, "coef", None),
            P(None, "coef", None),
            P(None, "cells"),
            P("cells"),
            P("coef", "cells"),
        ),
        out_specs=(P("coef", "cells"), P("cells")),
        check_vma=False,
    )
```

```python
import functools

import jax
import jax.numpy as jnp
from jax import lax
from jax.experimental import pallas as pl
from jax.experimental.pallas import tpu as pltpu
from jax.sharding import PartitionSpec as P

REACH = 2
WINDOWS = tuple(w for r in range(REACH, 0, -1) for w in (-r, r))
GROUP = 16
NT = (((1,), (1,)), ((), ()))


def halves(value):
    high = value.astype(jnp.bfloat16)
    low = (value - high.astype(jnp.float32)).astype(jnp.bfloat16)
    return high, low


def kernel(
    n_cells, n_coef,
    poles_hbm, parents_hbm, ops_hbm, l2l_hbm, target_hbm, leaf_hbm, basis_hbm,
    local_ref, pot_ref,
    ops_ref, l2l_ref, target_ref, leaf_ref, basis_ref,
    gathered, elders, pieces, out_buf, in_buf, total, partials,
    load_sem, g_send, g_recv, e_send, e_recv, w_send, w_recv, p_send, p_recv,
):
    row = lax.axis_index("cells")
    col = lax.axis_index("coef")
    noff, share, width = ops_ref.shape
    cd = target_ref.shape[1]
    tiles = leaf_ref.shape[0]
    lanes = leaf_ref.shape[1]

    loads = [
        pltpu.make_async_copy(src, dst, load_sem.at[i])
        for i, (src, dst) in enumerate(
            ((target_hbm, target_ref), (ops_hbm, ops_ref), (l2l_hbm, l2l_ref),
             (leaf_hbm, leaf_ref), (basis_hbm, basis_ref),
             (poles_hbm, gathered.at[col]), (parents_hbm, elders.at[col]))
        )
    ]
    for load in loads:
        load.start()

    barrier = pltpu.get_barrier_semaphore()
    for d in range(1, n_coef):
        pl.semaphore_signal(
            barrier, inc=1, device_id=(row, lax.rem(col + d, n_coef)),
            device_id_type=pl.DeviceIdType.MESH,
        )
    for w in WINDOWS:
        @pl.when((row + w >= 0) & (row + w < n_cells))
        def _():
            pl.semaphore_signal(
                barrier, inc=1, device_id=(row + w, col), device_id_type=pl.DeviceIdType.MESH
            )
    peers = n_coef - 1
    for w in WINDOWS:
        peers = peers + ((row + w >= 0) & (row + w < n_cells)).astype(jnp.int32)
    pl.semaphore_wait(barrier, peers)

    def gather_copy(k, d, slot):
        src, dst, send, recv = (
            (poles_hbm, gathered, g_send, g_recv), (parents_hbm, elders, e_send, e_recv)
        )[k]
        return pltpu.make_async_remote_copy(
            src_ref=src, dst_ref=dst.at[slot],
            send_sem=send.at[d - 1], recv_sem=recv.at[slot],
            device_id=(row, lax.rem(col + d, n_coef)), device_id_type=pl.DeviceIdType.MESH,
        )

    for k in range(2):
        for d in range(1, n_coef):
            gather_copy(k, d, col).start()
    loads[5].wait()
    loads[0].wait()
    for d in range(1, n_coef):
        gather_copy(0, d, lax.rem(col + d, n_coef)).wait_recv()
    loads[1].wait()

    poles = jnp.concatenate([gathered[j] for j in range(n_coef)], axis=0)
    iota = lax.broadcasted_iota(jnp.int32, (cd, cd), 0).astype(jnp.float32).astype(jnp.bfloat16)
    one = jnp.ones((cd, cd), jnp.bfloat16)
    zero = jnp.zeros((cd, cd), jnp.bfloat16)

    def one_hot(line):
        wide = jnp.broadcast_to(line.astype(jnp.float32), (16, line.shape[1])).astype(jnp.bfloat16)
        tall = jnp.concatenate([wide] * (cd // 16), axis=0)
        return jnp.where(tall == iota, one, zero)

    def lines(first, count):
        result = []
        for j in range(count):
            line = target_ref[pl.ds(first + j, 1), :]
            result.append(jnp.where(line >= 0, line - row * cd, -8 * REACH * cd))
        return result

    def span(first, count):
        return pl.ds(pl.multiple_of(first * cd, cd), count * cd)

    def far(first, count):
        block = ops_ref[pl.ds(first, count)].reshape(count * share, width)
        terms = jnp.dot(block, poles, preferred_element_type=jnp.float32)
        high, low = halves(terms)
        both = jnp.concatenate(
            [
                jnp.concatenate([part[j * share : (j + 1) * share] for j in range(count)], axis=1)
                for part in (high, low)
            ],
            axis=0,
        )
        pieces[:, span(first, count)] = both
        rows = lines(first, count)
        hot = jnp.concatenate(
            [
                jnp.concatenate([one_hot(line - w * cd) for line in rows], axis=1)
                for w in WINDOWS
            ],
            axis=0,
        )
        return lax.dot_general(both, hot, NT, preferred_element_type=jnp.float32)

    def near(first, count):
        hot = jnp.concatenate([one_hot(line) for line in lines(first, count)], axis=1)
        return lax.dot_general(
            pieces[:, span(first, count)], hot, NT, preferred_element_type=jnp.float32
        )

    def over_offsets(step, columns):
        full = noff // GROUP
        acc = jnp.zeros((2 * share, columns), jnp.float32)
        acc = lax.fori_loop(0, full, lambda i, a: a + step(i * GROUP, GROUP), acc)
        if noff % GROUP:
            acc = acc + step(full * GROUP, noff % GROUP)
        return acc[:share] + acc[share:]

    def window_copy(i, w):
        return pltpu.make_async_remote_copy(
            src_ref=out_buf.at[i], dst_ref=in_buf.at[i],
            send_sem=w_send.at[i], recv_sem=w_recv.at[i],
            device_id=(row + w, col), device_id_type=pl.DeviceIdType.MESH,
        )

    sums = over_offsets(far, len(WINDOWS) * cd)
    for i, w in enumerate(WINDOWS):
        out_buf[i] = sums[:, i * cd : (i + 1) * cd]
    for i, w in enumerate(WINDOWS):
        @pl.when((row + w >= 0) & (row + w < n_cells))
        def _():
            window_copy(i, w).start()

    total[...] = over_offsets(near, cd)

    loads[2].wait()
    loads[6].wait()
    for d in range(1, n_coef):
        gather_copy(1, d, lax.rem(col + d, n_coef)).wait_recv()
    held = (elders.shape[1], cd)
    child = lax.broadcasted_iota(jnp.int32, held, 1)
    family = child // 8 == lax.broadcasted_iota(jnp.int32, held, 0)
    family = family.astype(jnp.float32).astype(jnp.bfloat16)
    wide_parents = jnp.concatenate(
        [
            lax.dot_general(
                elders[j], family, (((0,), (0,)), ((), ())), preferred_element_type=jnp.float32
            )
            for j in range(n_coef)
        ],
        axis=0,
    )
    octant = lax.broadcasted_iota(jnp.int32, wide_parents.shape, 1) % 8
    spread = jnp.concatenate(
        [jnp.where(octant == j, wide_parents, 0.0).astype(jnp.bfloat16) for j in range(8)], axis=0
    )
    shifts = jnp.concatenate([l2l_ref[j] for j in range(8)], axis=1)
    total[...] += jnp.dot(shifts, spread, preferred_element_type=jnp.float32)

    loads[3].wait()
    leaf_hot = jnp.concatenate(
        [one_hot(leaf_ref[t : t + 1, :] - row * cd) for t in range(tiles)], axis=1
    )
    loads[4].wait()

    for i, w in enumerate(WINDOWS):
        @pl.when((row - w >= 0) & (row - w < n_cells))
        def _():
            window_copy(i, w).wait_recv()
            total[...] += in_buf[i]

    local = total[...]
    local_ref[...] = local
    columns = jnp.dot(
        jnp.concatenate(halves(local), axis=0), leaf_hot, preferred_element_type=jnp.float32
    )
    columns = columns[:share] + columns[share:]
    partial = jnp.sum(columns * basis_ref[...].astype(jnp.float32), axis=0, keepdims=True)
    partials[col] = jnp.concatenate(
        [partial[:, t * lanes : (t + 1) * lanes] for t in range(tiles)], axis=0
    )

    def partial_copy(d, slot):
        return pltpu.make_async_remote_copy(
            src_ref=partials.at[slot], dst_ref=partials.at[slot],
            send_sem=p_send.at[d - 1], recv_sem=p_recv.at[slot],
            device_id=(row, lax.rem(col + d, n_coef)), device_id_type=pl.DeviceIdType.MESH,
        )

    for d in range(1, n_coef):
        partial_copy(d, col).start()
    for d in range(1, n_coef):
        partial_copy(d, lax.rem(col + d, n_coef)).wait_recv()
    potential = partials[0]
    for j in range(1, n_coef):
        potential = potential + partials[j]
    pot_ref[...] = potential

    for d in range(1, n_coef):
        gather_copy(0, d, col).wait_send()
        gather_copy(1, d, col).wait_send()
        partial_copy(d, col).wait_send()
    for i, w in enumerate(WINDOWS):
        @pl.when((row + w >= 0) & (row + w < n_cells))
        def _():
            window_copy(i, w).wait_send()


def on_device(
    n_cells, n_coef,
    multipole, parent_local, m2l_ops, l2l_ops, target_cell, particle_leaf, particle_basis,
):
    share, cd = multipole.shape
    noff = m2l_ops.shape[0]
    width = m2l_ops.shape[2]
    particles = particle_leaf.shape[0]
    lanes = 128
    tiles = particles // lanes
    leaf = particle_leaf.reshape(tiles, lanes)
    nwin = len(WINDOWS)
    dma = pltpu.SemaphoreType.DMA
    vmem = pl.BlockSpec(memory_space=pltpu.VMEM)
    hbm = pl.BlockSpec(memory_space=pltpu.HBM)
    local, potential = pl.pallas_call(
        functools.partial(kernel, n_cells, n_coef),
        out_shape=(
            jax.ShapeDtypeStruct((share, cd), jnp.float32),
            jax.ShapeDtypeStruct((tiles, lanes), jnp.float32),
        ),
        in_specs=[hbm] * 7,
        out_specs=(vmem, vmem),
        scratch_shapes=[
            pltpu.VMEM(m2l_ops.shape, m2l_ops.dtype),
            pltpu.VMEM(l2l_ops.shape, l2l_ops.dtype),
            pltpu.VMEM(target_cell.shape, target_cell.dtype),
            pltpu.VMEM(leaf.shape, leaf.dtype),
            pltpu.VMEM(particle_basis.shape, particle_basis.dtype),
            pltpu.VMEM((n_coef, share, cd), jnp.bfloat16),
            pltpu.VMEM((n_coef,) + parent_local.shape[::-1], jnp.bfloat16),
            pltpu.VMEM((2 * share, noff * cd), jnp.bfloat16),
            pltpu.VMEM((nwin, share, cd), jnp.float32),
            pltpu.VMEM((nwin, share, cd), jnp.float32),
            pltpu.VMEM((share, cd), jnp.float32),
            pltpu.VMEM((n_coef, tiles, lanes), jnp.float32),
            dma((7,)),
            dma((n_coef - 1,)),
            dma((n_coef,)),
            dma((n_coef - 1,)),
            dma((n_coef,)),
            dma((nwin,)),
            dma((nwin,)),
            dma((n_coef - 1,)),
            dma((n_coef,)),
        ],
        compiler_params=pltpu.CompilerParams(
            collective_id=0, has_side_effects=True, vmem_limit_bytes=67043328
        ),
    )(multipole, parent_local.T, m2l_ops, l2l_ops, target_cell, leaf, particle_basis)
    return local, potential.reshape(particles)


def solution(mesh):
    return jax.shard_map(
        functools.partial(on_device, mesh.shape["cells"], mesh.shape["coef"]),
        mesh=mesh,
        in_specs=(
            P("coef", "cells"),
            P("coef", "cells"),
            P(None, "coef", None),
            P(None, "coef", None),
            P(None, "cells"),
            P("cells"),
            P("coef", "cells"),
        ),
        out_specs=(P("coef", "cells"), P("cells")),
        check_vma=False,
    )
```

```python
import functools

import jax
import jax.numpy as jnp
from jax import lax
from jax.experimental import pallas as pl
from jax.experimental.pallas import tpu as pltpu
from jax.sharding import PartitionSpec as P

REACH = 2
WINDOWS = tuple(w for r in range(REACH, 0, -1) for w in (-r, r))
GROUP = 16
NT = (((1,), (1,)), ((), ()))


def halves(value):
    high = value.astype(jnp.bfloat16)
    low = (value - high.astype(jnp.float32)).astype(jnp.bfloat16)
    return high, low


def kernel(
    n_cells, n_coef,
    poles_hbm, parents_hbm, ops_hbm, l2l_hbm, target_hbm, leaf_hbm, basis_hbm,
    local_ref, pot_ref,
    ops_ref, l2l_ref, target_ref, leaf_ref, basis_ref,
    gathered, elders, window_ref, hot_ref, leaf_hot_ref, pieces, out_buf, in_buf, total, partials,
    load_sem, g_send, g_recv, e_send, e_recv, w_send, w_recv, p_send, p_recv,
):
    row = lax.axis_index("cells")
    col = lax.axis_index("coef")
    noff, share, width = ops_ref.shape
    cd = target_ref.shape[1]
    tiles = leaf_ref.shape[0]
    lanes = leaf_ref.shape[1]

    loads = [
        pltpu.make_async_copy(src, dst, load_sem.at[i])
        for i, (src, dst) in enumerate(
            ((target_hbm, target_ref), (ops_hbm, ops_ref), (l2l_hbm, l2l_ref),
             (leaf_hbm, leaf_ref), (basis_hbm, basis_ref),
             (poles_hbm, gathered.at[col]), (parents_hbm, elders.at[col]))
        )
    ]
    for load in loads:
        load.start()

    barrier = pltpu.get_barrier_semaphore()
    for d in range(1, n_coef):
        pl.semaphore_signal(
            barrier, inc=1, device_id=(row, lax.rem(col + d, n_coef)),
            device_id_type=pl.DeviceIdType.MESH,
        )
    for w in WINDOWS:
        @pl.when((row + w >= 0) & (row + w < n_cells))
        def _():
            pl.semaphore_signal(
                barrier, inc=1, device_id=(row + w, col), device_id_type=pl.DeviceIdType.MESH
            )
    peers = n_coef - 1
    for w in WINDOWS:
        peers = peers + ((row + w >= 0) & (row + w < n_cells)).astype(jnp.int32)
    pl.semaphore_wait(barrier, peers)

    def gather_copy(k, d, slot):
        src, dst, send, recv = (
            (poles_hbm, gathered, g_send, g_recv), (parents_hbm, elders, e_send, e_recv)
        )[k]
        return pltpu.make_async_remote_copy(
            src_ref=src, dst_ref=dst.at[slot],
            send_sem=send.at[d - 1], recv_sem=recv.at[slot],
            device_id=(row, lax.rem(col + d, n_coef)), device_id_type=pl.DeviceIdType.MESH,
        )

    for k in range(2):
        for d in range(1, n_coef):
            gather_copy(k, d, col).start()
    iota = lax.broadcasted_iota(jnp.int32, (cd, cd), 0).astype(jnp.float32).astype(jnp.bfloat16)
    one = jnp.ones((cd, cd), jnp.bfloat16)
    zero = jnp.zeros((cd, cd), jnp.bfloat16)

    def one_hot(line):
        wide = jnp.broadcast_to(line.astype(jnp.float32), (16, line.shape[1])).astype(jnp.bfloat16)
        tall = jnp.concatenate([wide] * (cd // 16), axis=0)
        return jnp.where(tall == iota, one, zero)

    def span(first, count):
        return pl.ds(pl.multiple_of(first * cd, cd), count * cd)

    loads[0].wait()
    targets = target_ref[...] - row * cd
    window = targets // cd
    window_ref[...] = jnp.where(target_ref[...] >= 0, window, 8 * REACH).astype(jnp.float32)
    target_ref[...] = targets - window * cd

    def fill(first, count):
        hot_ref[:, span(first, count)] = jnp.concatenate(
            [one_hot(target_ref[pl.ds(first + j, 1), :]) for j in range(count)], axis=1
        )

    full = noff // GROUP
    lax.fori_loop(0, full, lambda i, _: fill(i * GROUP, GROUP), None)
    if noff % GROUP:
        fill(full * GROUP, noff % GROUP)

    loads[3].wait()
    leaf_hot_ref[...] = jnp.concatenate(
        [one_hot(leaf_ref[t : t + 1, :] - row * cd) for t in range(tiles)], axis=1
    )

    loads[5].wait()
    for d in range(1, n_coef):
        gather_copy(0, d, lax.rem(col + d, n_coef)).wait_recv()
    loads[1].wait()

    poles = jnp.concatenate([gathered[j] for j in range(n_coef)], axis=0)
    def far(first, count):
        block = ops_ref[pl.ds(first, count)].reshape(count * share, width)
        terms = jnp.dot(block, poles, preferred_element_type=jnp.float32)
        high, low = halves(terms)
        both = [
            jnp.concatenate([part[j * share : (j + 1) * share] for part in (high, low)], axis=0)
            for j in range(count)
        ]
        pieces[:, span(first, count)] = jnp.concatenate(both, axis=1)
        masked = [[] for _ in WINDOWS]
        for j in range(count):
            line = window_ref[pl.ds(first + j, 1), :]
            wide = jnp.broadcast_to(line, (16, cd)).astype(jnp.bfloat16)
            for i, w in enumerate(WINDOWS):
                keep = jnp.where(wide == w, one[:16], zero[:16])
                tall = jnp.concatenate([keep] * (2 * share // 16), axis=0)
                masked[i].append(both[j] * tall)
        stacked = jnp.concatenate([jnp.concatenate(m, axis=1) for m in masked], axis=0)
        return lax.dot_general(
            stacked, hot_ref[:, span(first, count)], NT, preferred_element_type=jnp.float32
        )

    def near(first, count):
        kept = []
        for j in range(count):
            line = window_ref[pl.ds(first + j, 1), :]
            wide = jnp.broadcast_to(line, (16, cd)).astype(jnp.bfloat16)
            keep = jnp.where(wide == 0, one[:16], zero[:16])
            tall = jnp.concatenate([keep] * (2 * share // 16), axis=0)
            kept.append(pieces[:, span(first + j, 1)] * tall)
        return lax.dot_general(
            jnp.concatenate(kept, axis=1), hot_ref[:, span(first, count)], NT,
            preferred_element_type=jnp.float32,
        )

    def over_offsets(step, rows):
        acc = jnp.zeros((rows, cd), jnp.float32)
        acc = lax.fori_loop(0, full, lambda i, a: a + step(i * GROUP, GROUP), acc)
        if noff % GROUP:
            acc = acc + step(full * GROUP, noff % GROUP)
        return acc

    def window_copy(i, w):
        return pltpu.make_async_remote_copy(
            src_ref=out_buf.at[i], dst_ref=in_buf.at[i],
            send_sem=w_send.at[i], recv_sem=w_recv.at[i],
            device_id=(row + w, col), device_id_type=pl.DeviceIdType.MESH,
        )

    sums = over_offsets(far, len(WINDOWS) * 2 * share)
    for i, w in enumerate(WINDOWS):
        base = 2 * share * i
        out_buf[i] = sums[base : base + share] + sums[base + share : base + 2 * share]
    for i, w in enumerate(WINDOWS):
        @pl.when((row + w >= 0) & (row + w < n_cells))
        def _():
            window_copy(i, w).start()

    sums = over_offsets(near, 2 * share)
    total[...] = sums[:share] + sums[share:]

    loads[2].wait()
    loads[6].wait()
    for d in range(1, n_coef):
        gather_copy(1, d, lax.rem(col + d, n_coef)).wait_recv()
    held = (elders.shape[1], cd)
    child = lax.broadcasted_iota(jnp.int32, held, 1)
    family = child // 8 == lax.broadcasted_iota(jnp.int32, held, 0)
    family = family.astype(jnp.float32).astype(jnp.bfloat16)
    wide_parents = jnp.concatenate(
        [
            lax.dot_general(
                elders[j], family, (((0,), (0,)), ((), ())), preferred_element_type=jnp.float32
            )
            for j in range(n_coef)
        ],
        axis=0,
    )
    octant = lax.broadcasted_iota(jnp.int32, wide_parents.shape, 1) % 8
    spread = jnp.concatenate(
        [jnp.where(octant == j, wide_parents, 0.0).astype(jnp.bfloat16) for j in range(8)], axis=0
    )
    shifts = jnp.concatenate([l2l_ref[j] for j in range(8)], axis=1)
    total[...] += jnp.dot(shifts, spread, preferred_element_type=jnp.float32)

    loads[4].wait()

    for i, w in enumerate(WINDOWS):
        @pl.when((row - w >= 0) & (row - w < n_cells))
        def _():
            window_copy(i, w).wait_recv()
            total[...] += in_buf[i]

    local = total[...]
    local_ref[...] = local
    columns = jnp.dot(
        jnp.concatenate(halves(local), axis=0), leaf_hot_ref[...], preferred_element_type=jnp.float32
    )
    columns = columns[:share] + columns[share:]
    partial = jnp.sum(columns * basis_ref[...].astype(jnp.float32), axis=0, keepdims=True)
    partials[col] = jnp.concatenate(
        [partial[:, t * lanes : (t + 1) * lanes] for t in range(tiles)], axis=0
    )

    def partial_copy(d, slot):
        return pltpu.make_async_remote_copy(
            src_ref=partials.at[slot], dst_ref=partials.at[slot],
            send_sem=p_send.at[d - 1], recv_sem=p_recv.at[slot],
            device_id=(row, lax.rem(col + d, n_coef)), device_id_type=pl.DeviceIdType.MESH,
        )

    for d in range(1, n_coef):
        partial_copy(d, col).start()
    for d in range(1, n_coef):
        partial_copy(d, lax.rem(col + d, n_coef)).wait_recv()
    potential = partials[0]
    for j in range(1, n_coef):
        potential = potential + partials[j]
    pot_ref[...] = potential

    for d in range(1, n_coef):
        gather_copy(0, d, col).wait_send()
        gather_copy(1, d, col).wait_send()
        partial_copy(d, col).wait_send()
    for i, w in enumerate(WINDOWS):
        @pl.when((row + w >= 0) & (row + w < n_cells))
        def _():
            window_copy(i, w).wait_send()


def on_device(
    n_cells, n_coef,
    multipole, parent_local, m2l_ops, l2l_ops, target_cell, particle_leaf, particle_basis,
):
    share, cd = multipole.shape
    noff = m2l_ops.shape[0]
    width = m2l_ops.shape[2]
    particles = particle_leaf.shape[0]
    lanes = 128
    tiles = particles // lanes
    leaf = particle_leaf.reshape(tiles, lanes)
    nwin = len(WINDOWS)
    dma = pltpu.SemaphoreType.DMA
    vmem = pl.BlockSpec(memory_space=pltpu.VMEM)
    hbm = pl.BlockSpec(memory_space=pltpu.HBM)
    local, potential = pl.pallas_call(
        functools.partial(kernel, n_cells, n_coef),
        out_shape=(
            jax.ShapeDtypeStruct((share, cd), jnp.float32),
            jax.ShapeDtypeStruct((tiles, lanes), jnp.float32),
        ),
        in_specs=[hbm] * 7,
        out_specs=(vmem, vmem),
        scratch_shapes=[
            pltpu.VMEM(m2l_ops.shape, m2l_ops.dtype),
            pltpu.VMEM(l2l_ops.shape, l2l_ops.dtype),
            pltpu.VMEM(target_cell.shape, target_cell.dtype),
            pltpu.VMEM(leaf.shape, leaf.dtype),
            pltpu.VMEM(particle_basis.shape, particle_basis.dtype),
            pltpu.VMEM((n_coef, share, cd), jnp.bfloat16),
            pltpu.VMEM((n_coef,) + parent_local.shape[::-1], jnp.bfloat16),
            pltpu.VMEM(target_cell.shape, jnp.float32),
            pltpu.VMEM((cd, noff * cd), jnp.bfloat16),
            pltpu.VMEM((cd, particles), jnp.bfloat16),
            pltpu.VMEM((2 * share, noff * cd), jnp.bfloat16),
            pltpu.VMEM((nwin, share, cd), jnp.float32),
            pltpu.VMEM((nwin, share, cd), jnp.float32),
            pltpu.VMEM((share, cd), jnp.float32),
            pltpu.VMEM((n_coef, tiles, lanes), jnp.float32),
            dma((7,)),
            dma((n_coef - 1,)),
            dma((n_coef,)),
            dma((n_coef - 1,)),
            dma((n_coef,)),
            dma((nwin,)),
            dma((nwin,)),
            dma((n_coef - 1,)),
            dma((n_coef,)),
        ],
        compiler_params=pltpu.CompilerParams(
            collective_id=0, has_side_effects=True, vmem_limit_bytes=67043328
        ),
    )(multipole, parent_local.T, m2l_ops, l2l_ops, target_cell, leaf, particle_basis)
    return local, potential.reshape(particles)


def solution(mesh):
    return jax.shard_map(
        functools.partial(on_device, mesh.shape["cells"], mesh.shape["coef"]),
        mesh=mesh,
        in_specs=(
            P("coef", "cells"),
            P("coef", "cells"),
            P(None, "coef", None),
            P(None, "coef", None),
            P(None, "cells"),
            P("cells"),
            P("coef", "cells"),
        ),
        out_specs=(P("coef", "cells"), P("cells")),
        check_vma=False,
    )
```
